16 devices in a mesh: dp: 4 (over z, y), tp: 4 (over x, core).
Axes of the slice: x: 2, y: 2, z: 2, core: 2. Of those that a mesh axis runs over, the one named last changes fastest.
Arguments:
- hidden: bfloat16 [64, 1024], P('dp'), parts along dimension 0
- lengths: int32 [64], P('dp'), parts along dimension 0
- choice: int32 [2, 64, 8], P(None, 'dp'), parts along dimension 1
- keys_one: bfloat16 [64, 64, 8, 64], P('dp', 'tp'), parts along dimension 0
- vals_one: bfloat16 [64, 64, 8, 64], P('dp', 'tp'), parts along dimension 0
- keys_two: bfloat16 [64, 64, 8, 64], P('dp', 'tp'), parts along dimension 0
- vals_two: bfloat16 [64, 64, 8, 64], P('dp', 'tp'), parts along dimension 0
- g_attn: bfloat16 [2, 1024], replicated
- w_q: bfloat16 [2, 1024, 1024], P(None, None, 'tp')
- w_k: bfloat16 [2, 1024, 512], P(None, None, 'tp')
- w_v: bfloat16 [2, 1024, 512], P(None, None, 'tp')
- w_o: bfloat16 [2, 1024, 1024], P(None, 'tp')
- g_mlp: bfloat16 [2, 1024], replicated
- w_router: bfloat16 [2, 1024, 32], replicated
- w_gate: bfloat16 [2, 32, 1024, 512], P(None, None, None, 'tp')
- w_up: bfloat16 [2, 32, 1024, 512], P(None, None, None, 'tp')
- w_down: bfloat16 [2, 32, 512, 1024], P(None, None, 'tp')
Outputs:
- output 1: bfloat16 [64, 1024], P('dp'), parts along dimension 0
- output 2: bfloat16 [64, 64, 8, 64], P('dp', None, 'tp'), parts along dimension 0
- output 3: bfloat16 [64, 64, 8, 64], P('dp', None, 'tp'), parts along dimension 0
- output 4: bfloat16 [64, 64, 8, 64], P('dp', None, 'tp'), parts along dimension 0
- output 5: bfloat16 [64, 64, 8, 64], P('dp', None, 'tp'), parts along dimension 0
There are 4 independent parts. The reference program is written for one: setup_inputs(seed, part) draws one part's arguments, and reference() takes and returns one part's arrays. A program takes and returns all parts, laid end to end along the dimension named above; an argument that names none is the same for every part.
All inputs are finite; a program needn't handle non-finite values.
Results may differ from the reference program's by a relative error of at most 0.02.
Values are sent between devices in bfloat16 or wider.
A program may use at most 1 GiB of HBM per device.

```python
import jax
import jax.numpy as jnp
from jax import lax

BATCH = 16
SEQ = 64
D = 1024
HEADS = 16
KV_HEADS = 8
HEAD = 64
FF = 512
EXPERTS = 32
TOP = 8
LAYERS = 2
EPS = 1e-5
THETA = 1000000.0


def weight_draw(key, shape, fan_in, gain_mult):
    return (jax.random.normal(key, shape, jnp.float32) * (gain_mult * fan_in ** -0.5)).astype(jnp.bfloat16)


def value_walk(key, cache_shape):
    step_key, noise_key = jax.random.split(key)
    walk_steps = jax.random.normal(step_key, cache_shape, jnp.float32) * SEQ ** -0.5
    noise_part = 0.5 * jax.random.normal(noise_key, cache_shape, jnp.float32)
    return (jnp.cumsum(walk_steps, axis=1) + noise_part).astype(jnp.bfloat16)


def setup_inputs(seed: int = 0, part: int = 0) -> dict:
    base_key = jax.random.key(seed)
    shared = jax.random.split(base_key, 11)
    local_keys = jax.random.split(jax.random.fold_in(base_key, part), 9)
    cache_shape = (BATCH, SEQ, KV_HEADS, HEAD)
    hidden = jax.random.normal(local_keys[0], (BATCH, D), jnp.float32).astype(jnp.bfloat16)
    drawn_lens = jax.random.randint(local_keys[1], (BATCH,), 0, SEQ)
    full_row = jax.random.randint(local_keys[2], (), 0, BATCH)
    lengths = jnp.where(jnp.arange(BATCH) == full_row, SEQ - 1, drawn_lens).astype(jnp.int32)
    rank_score = jax.random.randint(local_keys[3], (LAYERS, BATCH, EXPERTS), 0, 2 ** 20) * EXPERTS + jnp.arange(EXPERTS)
    choice = lax.top_k(rank_score, TOP)[1].astype(jnp.int32)
    return {
        'hidden': hidden,
        'lengths': lengths,
        'choice': choice,
        'keys_one': jax.random.normal(local_keys[4], cache_shape, jnp.float32).astype(jnp.bfloat16),
        'vals_one': value_walk(local_keys[5], cache_shape),
        'keys_two': jax.random.normal(local_keys[6], cache_shape, jnp.float32).astype(jnp.bfloat16),
        'vals_two': value_walk(local_keys[7], cache_shape),
        'g_attn': (1.0 + 0.3 * jax.random.normal(shared[0], (LAYERS, D), jnp.float32)).astype(jnp.bfloat16),
        'w_q': weight_draw(shared[1], (LAYERS, D, HEADS * HEAD), D, 1.0),
        'w_k': weight_draw(shared[2], (LAYERS, D, KV_HEADS * HEAD), D, 1.0),
        'w_v': weight_draw(shared[3], (LAYERS, D, KV_HEADS * HEAD), D, 1.0),
        'w_o': weight_draw(shared[4], (LAYERS, HEADS * HEAD, D), HEADS * HEAD, 1.0),
        'g_mlp': (1.0 + 0.3 * jax.random.normal(shared[5], (LAYERS, D), jnp.float32)).astype(jnp.bfloat16),
        'w_router': weight_draw(shared[6], (LAYERS, D, EXPERTS), D, 2.0),
        'w_gate': weight_draw(shared[7], (LAYERS, EXPERTS, D, FF), D, 1.0),
        'w_up': weight_draw(shared[8], (LAYERS, EXPERTS, D, FF), D, 1.0),
        'w_down': weight_draw(shared[9], (LAYERS, EXPERTS, FF, D), FF, 2.0),
    }


def rms_norm(tensor, gain_vec):
    tensor_f = tensor.astype(jnp.float32)
    scale = lax.rsqrt(jnp.mean(tensor_f * tensor_f, axis=-1, keepdims=True) + EPS)
    return (tensor_f * scale * gain_vec.astype(jnp.float32)).astype(jnp.bfloat16)


def apply_rope(tensor, lengths):
    head_dim = tensor.shape[-1]
    half_dim = head_dim // 2
    inv_freq = THETA ** (-2.0 * jnp.arange(half_dim, dtype=jnp.float32) / head_dim)
    angle = lengths.astype(jnp.float32)[:, None] * inv_freq[None, :]
    cos_part = jnp.cos(angle)[:, None, :]
    sin_part = jnp.sin(angle)[:, None, :]
    lower_half = tensor[..., :half_dim]
    upper_half = tensor[..., half_dim:]
    return jnp.concatenate([lower_half * cos_part - upper_half * sin_part, upper_half * cos_part + lower_half * sin_part], axis=-1)


def decode_layer(hidden, lengths, choice, key_cache, val_cache, g_attn, w_q, w_k, w_v, w_o, g_mlp, w_router, w_gate, w_up, w_down):
    batch_rows = hidden.shape[0]
    seq_len = key_cache.shape[1]
    normed = rms_norm(hidden, g_attn)
    query_rot = apply_rope(jnp.dot(normed, w_q, preferred_element_type=jnp.float32).reshape(batch_rows, HEADS, HEAD), lengths).astype(jnp.bfloat16)
    key_new = apply_rope(jnp.dot(normed, w_k, preferred_element_type=jnp.float32).reshape(batch_rows, KV_HEADS, HEAD), lengths).astype(jnp.bfloat16)
    val_new = jnp.dot(normed, w_v, preferred_element_type=jnp.float32).astype(jnp.bfloat16).reshape(batch_rows, KV_HEADS, HEAD)
    positions = jnp.arange(seq_len)
    is_new = (positions[None, :] == lengths[:, None])[:, :, None, None]
    key_cache = jnp.where(is_new, key_new[:, None], key_cache)
    val_cache = jnp.where(is_new, val_new[:, None], val_cache)
    query_grp = query_rot.reshape(batch_rows, KV_HEADS, HEADS // KV_HEADS, HEAD)
    scores = jnp.einsum('bgrd,bsgd->bgrs', query_grp.astype(jnp.float32), key_cache.astype(jnp.float32)) * HEAD ** -0.5
    is_valid = (positions[None, :] <= lengths[:, None])[:, None, None, :]
    attn_prob = jax.nn.softmax(jnp.where(is_valid, scores, -1e30), axis=-1).astype(jnp.bfloat16)
    attn_vec = jnp.einsum('bgrs,bsgd->bgrd', attn_prob.astype(jnp.float32), val_cache.astype(jnp.float32)).astype(jnp.bfloat16).reshape(batch_rows, HEADS * HEAD)
    x_mid = (hidden.astype(jnp.float32) + jnp.dot(attn_vec, w_o, preferred_element_type=jnp.float32)).astype(jnp.bfloat16)
    normed_mid = rms_norm(x_mid, g_mlp)
    logits = jnp.dot(normed_mid, w_router, preferred_element_type=jnp.float32)
    onehot = (choice[:, :, None] == jnp.arange(EXPERTS)[None, None, :]).astype(jnp.float32)
    gate_prob = jax.nn.softmax(jnp.sum(onehot * logits[:, None, :], axis=-1), axis=-1)
    gate_mat = jnp.sum(gate_prob[:, :, None] * onehot, axis=1)
    gate_act = jnp.einsum('bd,edf->bef', normed_mid.astype(jnp.float32), w_gate.astype(jnp.float32))
    up_act = jnp.einsum('bd,edf->bef', normed_mid.astype(jnp.float32), w_up.astype(jnp.float32))
    expert_in = (jax.nn.silu(gate_act) * up_act * gate_mat[:, :, None]).astype(jnp.bfloat16)
    moe_out = jnp.einsum('bef,efd->bd', expert_in.astype(jnp.float32), w_down.astype(jnp.float32))
    return (x_mid.astype(jnp.float32) + moe_out).astype(jnp.bfloat16), key_cache, val_cache


def reference(hidden, lengths, choice, keys_one, vals_one, keys_two, vals_two, g_attn, w_q, w_k, w_v, w_o, g_mlp, w_router, w_gate, w_up, w_down):
    caches = [(keys_one, vals_one), (keys_two, vals_two)]
    results = []
    for layer_idx in range(LAYERS):
        hidden, key_cache, val_cache = decode_layer(hidden, lengths, choice[layer_idx], caches[layer_idx][0], caches[layer_idx][1], g_attn[layer_idx], w_q[layer_idx], w_k[layer_idx], w_v[layer_idx], w_o[layer_idx], g_mlp[layer_idx], w_router[layer_idx], w_gate[layer_idx], w_up[layer_idx], w_down[layer_idx])
        results.append(key_cache)
        results.append(val_cache)
    return (hidden, results[0], results[1], results[2], results[3])
```

```python
import math

import jax
import jax.numpy as jnp
from jax import lax
from jax.experimental import pallas as pl
from jax.experimental.pallas import tpu as pltpu
from jax.sharding import PartitionSpec as P

EPS = 1e-5
THETA = 1000000.0
LAYERS = 2
B = 16
SEQ = 64
D = 1024
HEAD = 64
EXPERTS = 32
TP = 4
LOCAL = SEQ // TP
CHUNKS = 4
CB = B // CHUNKS
WCH = 8
EPC = EXPERTS // WCH
NCH = 4
NW = D // NCH
BF = jnp.bfloat16
F32 = jnp.float32
MESH = pl.DeviceIdType.MESH
NT = (((1,), (1,)), ((), ()))


def dot(a, b):
    return jnp.dot(a, b, preferred_element_type=F32)


def dot_nt(a, b):
    return lax.dot_general(a, b, NT, preferred_element_type=F32)


def iota(shape, dim):
    return lax.broadcasted_iota(jnp.int32, shape, dim)


def kernel(lens, hid, cho, k1, v1, k2, v2, ga, wq, wk, wv, wo, gm, wr, wg, wu, wd,
           h_out, ko1, vo1, ko2, vo2,
           lens_s, hid_b, cho_b, ga_b, gm_b, wq_b, wk_b, wv_b, wo_b, wr_b, wg_b, wu_b, wd_b,
           kin, stage, send, recv, istage, kst, vst, kvn, ar, ub, hst,
           sm, cs, ws, es, ss, rs, ass, ars, osem):
    me = lax.axis_index('tp')
    peers = {1: me + 1 - 2 * (me % 2), 2: (me + 2) % 4, 3: 3 - me}
    caches = ((k1, v1), (k2, v2))
    outs = ((ko1, vo1), (ko2, vo2))

    def cache_in(l, kv, c):
        sl = pl.ds(c * CB, CB)
        return pltpu.make_async_copy(caches[l][kv].at[sl], kin.at[l, kv, sl], cs.at[l, kv, c])

    smalls = [pltpu.make_async_copy(s, d, sm.at[i]) for i, (s, d) in enumerate(
        ((lens, lens_s), (hid, hid_b), (cho, cho_b), (ga, ga_b), (gm, gm_b), (wr, wr_b)))]

    def proj_in(l):
        return [pltpu.make_async_copy(s.at[l], d.at[l], ws.at[l, i]) for i, (s, d) in enumerate(
            ((wq, wq_b), (wk, wk_b), (wv, wv_b), (wo, wo_b)))]

    def expert_in(l, c):
        sl = pl.ds(c * EPC, EPC)
        rl = pl.ds(c * EPC * 128, EPC * 128)
        return [pltpu.make_async_copy(wg.at[l, sl], wg_b.at[l, sl], es.at[l, 0, c]),
                pltpu.make_async_copy(wu.at[l, sl], wu_b.at[l, sl], es.at[l, 1, c]),
                pltpu.make_async_copy(wd.at[l, rl], wd_b.at[l, rl], es.at[l, 2, c])]

    for c in range(CHUNKS):
        for kv in range(2):
            cache_in(0, kv, c).start()
    for cp in smalls + proj_in(0):
        cp.start()
    bar = pltpu.get_barrier_semaphore()
    for j in (1, 2, 3):
        pl.semaphore_signal(bar, inc=1, device_id={'tp': peers[j]}, device_id_type=MESH)
    for c in range(CHUNKS):
        for kv in range(2):
            cache_in(1, kv, c).start()
    for l in range(LAYERS):
        for c in range(WCH):
            for cp in expert_in(l, c):
                cp.start()
        if l == 0:
            for cp in proj_in(1):
                cp.start()
    pl.semaphore_wait(bar, 3)

    def kv_send(l, c, j):
        sl = pl.ds(c * CB, CB)
        return pltpu.make_async_remote_copy(
            send.at[l, peers[j], sl], recv.at[l, sl, me], ss.at[l, c, j - 1], rs.at[l, c, j - 1],
            device_id={'tp': peers[j]}, device_id_type=MESH)

    def kv_recv(l, c, j):
        sl = pl.ds(c * CB, CB)
        return pltpu.make_async_remote_copy(
            send.at[l, me, sl], recv.at[l, sl, peers[j]], ss.at[l, c, j - 1], rs.at[l, c, j - 1],
            device_id={'tp': peers[j]}, device_id_type=MESH)

    def pack_send(l):
        for c in range(CHUNKS):
            for kv in range(2):
                cache_in(l, kv, c).wait()
            sl = pl.ds(c * CB, CB)
            kf = kin[l, 0, sl].astype(F32).reshape(CB * LOCAL * 8, HEAD)
            vf = kin[l, 1, sl].astype(F32).reshape(CB * LOCAL * 8, HEAD)
            stage[...] = jnp.concatenate([kf, vf], axis=1)
            for h in range(8):
                rows = stage[pl.ds(h, CB * LOCAL, stride=8), :].astype(BF)
                send[l, h // 2, sl, h % 2] = rows.reshape(CB, LOCAL, 128)
            recv[l, sl, me] = send[l, me, sl]
            for j in (2, 3, 1):
                kv_send(l, c, j).start()

    def ar_copy(a, n, j, slot):
        return pltpu.make_async_remote_copy(
            ar.at[a, me, n], ar.at[a, slot, n], ass.at[a, n, j - 1], ars.at[a, n, j - 1],
            device_id={'tp': peers[j]}, device_id_type=MESH)

    def ar_send(a, n, value):
        ar[a, me, n] = value.astype(BF)
        for j in (2, 3, 1):
            ar_copy(a, n, j, me).start()

    def ar_sum(a, h):
        parts = []
        for n in range(NCH):
            for j in (1, 2, 3):
                ar_copy(a, n, j, peers[j]).wait_recv()
            tot = ar[a, 0, n].astype(F32)
            for s in range(1, TP):
                tot = tot + ar[a, s, n].astype(F32)
            parts.append(tot)
        return (h.astype(F32) + jnp.concatenate(parts, axis=1)).astype(BF)

    def rms(h, gain):
        hf = h.astype(F32)
        scale = lax.rsqrt(jnp.mean(hf * hf, axis=1, keepdims=True) + EPS)
        return (hf * scale * gain.astype(F32)).astype(BF)

    lane = iota((B, 128), 1)
    low = lane < HEAD

    def rope(x, cosv, sinv):
        rot = jnp.where((lane % HEAD) < HEAD // 2, pltpu.roll(x, 128 - HEAD // 2, 1), pltpu.roll(x, HEAD // 2, 1))
        return (x * cosv + rot * sinv).astype(BF).astype(F32)

    pack_send(0)
    for cp in smalls:
        cp.wait()
    lenv = jnp.zeros((B, 128), jnp.int32)
    rowi = iota((B, 128), 0)
    for b in range(B):
        lenv = jnp.where(rowi == b, lens_s[b], lenv)
    freq = jnp.exp((lane % (HEAD // 2)).astype(F32) * (-2.0 * math.log(THETA) / HEAD))
    ang = lenv.astype(F32) * freq
    cosv = jnp.cos(ang)
    sinv = jnp.sin(ang)
    sinv = jnp.where((lane % HEAD) < HEAD // 2, -sinv, sinv)

    row64 = iota((64, 128), 0)
    rowb = row64 % B
    col = iota((64, 128), 1)
    pos = (col // 32) * LOCAL + col % LOCAL
    same = ((col // LOCAL) % 2) == (row64 // 32)
    len64 = jnp.concatenate([lenv] * 4, axis=0)
    valid = same & (pos <= len64)
    isnew = same & (pos == len64)

    def attention(l, h):
        a = rms(h, ga_b[l:l + 1, :])
        for cp in proj_in(l):
            cp.wait()
        q = dot(a, wq_b[l])
        k = rope(dot(a, wk_b[l]), cosv, sinv)
        v = dot(a, wv_b[l]).astype(BF).astype(F32)
        new0 = jnp.where(low, k, pltpu.roll(v, HEAD, 1))
        new1 = jnp.where(low, pltpu.roll(k, HEAD, 1), v)
        kvn[l, 0] = new0
        kvn[l, 1] = new1
        qs = []
        for i in range(2):
            qi = rope(q[:, i * 128:(i + 1) * 128], cosv, sinv)
            qs.append(jnp.where(low, qi, 0.0))
            qs.append(jnp.where(low, pltpu.roll(qi, HEAD, 1), 0.0))
        qf = jnp.concatenate(qs, axis=0)
        newr = jnp.concatenate([new0, new0, new1, new1], axis=0)
        qb = qf.astype(BF)
        snew = jnp.sum(qf * newr, axis=1, keepdims=True)
        s = jnp.zeros((64, 128), F32)
        for c in range(CHUNKS):
            for j in (1, 2, 3):
                kv_recv(l, c, j).wait_recv()
            for b in range(c * CB, (c + 1) * CB, 2):
                kvb = recv[l, b:b + 2].reshape(256, 128)
                sb = dot_nt(qb, kvb)
                s = jnp.where(rowb == b, sb[:, :128], s)
                s = jnp.where(rowb == b + 1, sb[:, 128:], s)
        s = jnp.where(isnew, snew, s) * (HEAD ** -0.5)
        s = jnp.where(valid, s, -1e30)
        e = jnp.exp(s - jnp.max(s, axis=1, keepdims=True))
        p = (e / jnp.sum(e, axis=1, keepdims=True)).astype(BF).astype(F32)
        pn = jnp.sum(jnp.where(isnew, p, 0.0), axis=1, keepdims=True)
        p = jnp.where(isnew, 0.0, p)
        o = pn * newr
        for b in range(0, B, 2):
            pb = jnp.concatenate([jnp.where(rowb == b, p, 0.0), jnp.where(rowb == b + 1, p, 0.0)], axis=1).astype(BF)
            o = o + dot(pb, recv[l, b:b + 2].reshape(256, 128))
        att = jnp.concatenate(
            [jnp.where(low, pltpu.roll(o[32 * i:32 * i + 16], HEAD, 1), o[32 * i + 16:32 * i + 32]) for i in range(2)],
            axis=1).astype(BF)
        for n in range(NCH):
            ar_send(2 * l, n, dot(att, wo_b[l, :, n * NW:(n + 1) * NW]))

    def cache_out(l, kv):
        return pltpu.make_async_copy((kst, vst)[kv].at[l], outs[l][kv], osem.at[l, kv])

    def write_caches(l):
        row = iota((SEQ, 128), 0)

        def body(b, carry):
            kvb = recv[l, b].astype(F32)
            for g in range(2):
                x = kvb[:, g].reshape(SEQ, 128)
                x = jnp.where(row == lens_s[b], kvn[l, g, pl.ds(b, 1), :], x)
                istage[pl.ds(g, SEQ, stride=2), :] = x
            z = istage[...]
            kst[l, b] = z[:, :HEAD].astype(BF)
            vst[l, b] = z[:, HEAD:].astype(BF)
            return carry

        lax.fori_loop(0, B, body, 0)
        for kv in range(2):
            cache_out(l, kv).start()

    def gates(l, m):
        choice = cho_b[l]
        onehot = jnp.zeros((EXPERTS, B), F32)
        erow = iota((EXPERTS, B), 0)
        for j in range(8):
            onehot = onehot + (erow == choice[j:j + 1, :]).astype(F32)
        eye = (iota((B, B), 0) == iota((B, B), 1)).astype(BF)
        mask = dot_nt(eye, onehot.astype(BF)) > 0.5
        logits = jnp.where(mask, dot_nt(m, wr_b[l]), -1e30)
        ex = jnp.where(mask, jnp.exp(logits - jnp.max(logits, axis=1, keepdims=True)), 0.0)
        return ex / jnp.sum(ex, axis=1, keepdims=True)

    def experts(l, h1):
        m = rms(h1, gm_b[l:l + 1, :])
        gate = gates(l, m)
        for c in range(WCH):
            for cp in expert_in(l, c):
                cp.wait()
        for e in range(EXPERTS):
            acc = None
            for kk in range(4):
                ks = slice(kk * 256, (kk + 1) * 256)
                w = jnp.concatenate([wg_b[l, e, ks, :], wu_b[l, e, ks, :]], axis=1)
                t = dot(m[:, ks], w)
                acc = t if acc is None else acc + t
            ga_act, up = acc[:, :128], acc[:, 128:]
            act = ga_act * jax.nn.sigmoid(ga_act) * up * gate[:, e:e + 1]
            ub[:, e * 128:(e + 1) * 128] = act.astype(BF)
        for n in range(NCH):
            ar_send(2 * l + 1, n, dot(ub[...], wd_b[l, :, n * NW:(n + 1) * NW]))

    h = hid_b[...]
    for l in range(LAYERS):
        attention(l, h)
        if l == 0:
            pack_send(1)
        write_caches(l)
        h1 = ar_sum(2 * l, h)
        experts(l, h1)
        h = ar_sum(2 * l + 1, h1)
    hst[...] = h
    hcp = pltpu.make_async_copy(hst, h_out, sm.at[6])
    hcp.start()
    for l in range(LAYERS):
        for c in range(CHUNKS):
            for j in (1, 2, 3):
                kv_send(l, c, j).wait_send()
        for a in (2 * l, 2 * l + 1):
            for n in range(NCH):
                for j in (1, 2, 3):
                    ar_copy(a, n, j, me).wait_send()
        for kv in range(2):
            cache_out(l, kv).wait()
    hcp.wait()


def solution(mesh):
    seq_spec = P('dp', 'tp', None, None)
    head_spec = P('dp', None, 'tp', None)
    col_spec = P(None, None, 'tp')
    ff_spec = P(None, None, None, 'tp')
    anyspec = pl.BlockSpec(memory_space=pl.ANY)
    dma = pltpu.SemaphoreType.DMA

    def local_step(hidden, lengths, choice, keys_one, vals_one, keys_two, vals_two, g_attn, w_q, w_k, w_v, w_o, g_mlp, w_router, w_gate, w_up, w_down):
        cho = jnp.transpose(choice, (0, 2, 1))
        wr = jnp.transpose(w_router, (0, 2, 1))
        wd = w_down.reshape(LAYERS, EXPERTS * 128, D)
        cache_shape = jax.ShapeDtypeStruct((B, SEQ * 2, HEAD), BF)
        h, k1, v1, k2, v2 = pl.pallas_call(
            kernel,
            out_shape=(jax.ShapeDtypeStruct((B, D), BF),) + (cache_shape,) * 4,
            in_specs=[anyspec] * 17,
            out_specs=(anyspec,) * 5,
            scratch_shapes=[
                pltpu.SMEM((B,), jnp.int32),
                pltpu.VMEM((B, D), BF),
                pltpu.VMEM((LAYERS, 8, B), jnp.int32),
                pltpu.VMEM((LAYERS, D), BF),
                pltpu.VMEM((LAYERS, D), BF),
                pltpu.VMEM((LAYERS, D, 256), BF),
                pltpu.VMEM((LAYERS, D, 128), BF),
                pltpu.VMEM((LAYERS, D, 128), BF),
                pltpu.VMEM((LAYERS, 256, D), BF),
                pltpu.VMEM((LAYERS, EXPERTS, D), BF),
                pltpu.VMEM((LAYERS, EXPERTS, D, 128), BF),
                pltpu.VMEM((LAYERS, EXPERTS, D, 128), BF),
                pltpu.VMEM((LAYERS, EXPERTS * 128, D), BF),
                pltpu.VMEM((LAYERS, 2, B, LOCAL, 8, HEAD), BF),
                pltpu.VMEM((CB * LOCAL * 8, 128), F32),
                pltpu.VMEM((LAYERS, TP, B, 2, LOCAL, 128), BF),
                pltpu.VMEM((LAYERS, B, TP, 2, LOCAL, 128), BF),
                pltpu.VMEM((2 * SEQ, 128), F32),
                pltpu.VMEM((LAYERS, B, 2 * SEQ, HEAD), BF),
                pltpu.VMEM((LAYERS, B, 2 * SEQ, HEAD), BF),
                pltpu.VMEM((LAYERS, 2, B, 128), F32),
                pltpu.VMEM((2 * LAYERS, TP, NCH, B, NW), BF),
                pltpu.VMEM((B, EXPERTS * 128), BF),
                pltpu.VMEM((B, D), BF),
                dma((7,)),
                dma((LAYERS, 2, CHUNKS)),
                dma((LAYERS, 4)),
                dma((LAYERS, 3, WCH)),
                dma((LAYERS, CHUNKS, 3)),
                dma((LAYERS, CHUNKS, 3)),
                dma((2 * LAYERS, NCH, 3)),
                dma((2 * LAYERS, NCH, 3)),
                dma((LAYERS, 2)),
            ],
            compiler_params=pltpu.CompilerParams(collective_id=0, has_side_effects=True, vmem_limit_bytes=67_000_000),
            name='decode_two_layers',
        )(lengths, hidden, cho, keys_one, vals_one, keys_two, vals_two, g_attn, w_q, w_k, w_v, w_o, g_mlp, wr, w_gate, w_up, wd)
        shape = (B, SEQ, 2, HEAD)
        return (h, k1.reshape(shape), v1.reshape(shape), k2.reshape(shape), v2.reshape(shape))

    return jax.shard_map(local_step, mesh=mesh, in_specs=(P('dp', None), P('dp'), P(None, 'dp', None), seq_spec, seq_spec, seq_spec, seq_spec, P(), col_spec, col_spec, col_spec, P(None, 'tp', None), P(), P(), ff_spec, ff_spec, P(None, None, 'tp', None)), out_specs=(P('dp', None), head_spec, head_spec, head_spec, head_spec), check_vma=False)
```

```python
import math

import jax
import jax.numpy as jnp
from jax import lax
from jax.experimental import pallas as pl
from jax.experimental.pallas import tpu as pltpu
from jax.sharding import PartitionSpec as P

EPS = 1e-5
THETA = 1000000.0
LAYERS = 2
B = 16
SEQ = 64
D = 1024
HEAD = 64
EXPERTS = 32
TP = 4
LOCAL = SEQ // TP
CHUNKS = 4
CB = B // CHUNKS
WCH = 8
EPC = EXPERTS // WCH
NCH = 4
NW = D // NCH
BF = jnp.bfloat16
F32 = jnp.float32
MESH = pl.DeviceIdType.MESH
NT = (((1,), (1,)), ((), ()))


def dot(a, b):
    return jnp.dot(a, b, preferred_element_type=F32)


def dot_nt(a, b):
    return lax.dot_general(a, b, NT, preferred_element_type=F32)


def iota(shape, dim):
    return lax.broadcasted_iota(jnp.int32, shape, dim)


def kernel(lens, hid, cho, k1, v1, k2, v2, ga, wq, wk, wv, wo, gm, wr, wg, wu, wd,
           hst, ko1, vo1, ko2, vo2,
           lens_s, hid_b, cho_b, ga_b, gm_b, wq_b, wk_b, wv_b, wo_b, wr_b, wg_b, wu_b, wd_b,
           kin, stage, send, recv, istage, kvn, ar, ub,
           sm, cs, ws, es, ss, rs, ass, ars):
    me = lax.axis_index('tp')
    peers = {1: me + 1 - 2 * (me % 2), 2: (me + 2) % 4, 3: 3 - me}
    caches = ((k1, v1), (k2, v2))
    outs = ((ko1, vo1), (ko2, vo2))

    def cache_in(l, kv, c):
        sl = pl.ds(c * CB, CB)
        return pltpu.make_async_copy(caches[l][kv].at[sl], kin.at[l, kv, sl], cs.at[l, kv, c])

    smalls = [pltpu.make_async_copy(s, d, sm.at[i]) for i, (s, d) in enumerate(
        ((lens, lens_s), (hid, hid_b), (cho, cho_b), (ga, ga_b), (gm, gm_b), (wr, wr_b)))]

    def proj_in(l):
        return [pltpu.make_async_copy(s.at[l], d.at[l], ws.at[l, i]) for i, (s, d) in enumerate(
            ((wq, wq_b), (wk, wk_b), (wv, wv_b), (wo, wo_b)))]

    def expert_in(l, c):
        sl = pl.ds(c * EPC, EPC)
        rl = pl.ds(c * EPC * 128, EPC * 128)
        return [pltpu.make_async_copy(wg.at[l, sl], wg_b.at[l, sl], es.at[l, 0, c]),
                pltpu.make_async_copy(wu.at[l, sl], wu_b.at[l, sl], es.at[l, 1, c]),
                pltpu.make_async_copy(wd.at[l, rl], wd_b.at[l, rl], es.at[l, 2, c])]

    for c in range(CHUNKS):
        for kv in range(2):
            cache_in(0, kv, c).start()
    for cp in smalls + proj_in(0):
        cp.start()
    bar = pltpu.get_barrier_semaphore()
    for j in (1, 2, 3):
        pl.semaphore_signal(bar, inc=1, device_id={'tp': peers[j]}, device_id_type=MESH)
    for c in range(CHUNKS):
        for kv in range(2):
            cache_in(1, kv, c).start()
    for l in range(LAYERS):
        for c in range(WCH):
            for cp in expert_in(l, c):
                cp.start()
        if l == 0:
            for cp in proj_in(1):
                cp.start()
    pl.semaphore_wait(bar, 3)

    def kv_send(l, c, j):
        sl = pl.ds(c * CB, CB)
        return pltpu.make_async_remote_copy(
            send.at[l, peers[j], sl], recv.at[l, sl, me], ss.at[l, c, j - 1], rs.at[l, c, j - 1],
            device_id={'tp': peers[j]}, device_id_type=MESH)

    def kv_recv(l, c, j):
        sl = pl.ds(c * CB, CB)
        return pltpu.make_async_remote_copy(
            send.at[l, me, sl], recv.at[l, sl, peers[j]], ss.at[l, c, j - 1], rs.at[l, c, j - 1],
            device_id={'tp': peers[j]}, device_id_type=MESH)

    def pack_send(l):
        for c in range(CHUNKS):
            for kv in range(2):
                cache_in(l, kv, c).wait()
            sl = pl.ds(c * CB, CB)
            kf = kin[l, 0, sl].astype(F32).reshape(CB * LOCAL * 8, HEAD)
            vf = kin[l, 1, sl].astype(F32).reshape(CB * LOCAL * 8, HEAD)
            stage[...] = jnp.concatenate([kf, vf], axis=1)
            for h in range(8):
                rows = stage[pl.ds(h, CB * LOCAL, stride=8), :].astype(BF)
                send[l, h // 2, sl, h % 2] = rows.reshape(CB, LOCAL, 128)
            recv[l, sl, me] = send[l, me, sl]
            for j in (2, 3, 1):
                kv_send(l, c, j).start()

    def ar_copy(a, n, j, slot):
        return pltpu.make_async_remote_copy(
            ar.at[a, me, n], ar.at[a, slot, n], ass.at[a, n, j - 1], ars.at[a, n, j - 1],
            device_id={'tp': peers[j]}, device_id_type=MESH)

    def ar_send(a, n, value):
        ar[a, me, n] = value.astype(BF)
        for j in (2, 3, 1):
            ar_copy(a, n, j, me).start()

    def ar_sum(a, h):
        parts = []
        for n in range(NCH):
            for j in (1, 2, 3):
                ar_copy(a, n, j, peers[j]).wait_recv()
            tot = ar[a, 0, n].astype(F32)
            for s in range(1, TP):
                tot = tot + ar[a, s, n].astype(F32)
            parts.append(tot)
        return (h.astype(F32) + jnp.concatenate(parts, axis=1)).astype(BF)

    def rms(h, gain):
        hf = h.astype(F32)
        scale = lax.rsqrt(jnp.mean(hf * hf, axis=1, keepdims=True) + EPS)
        return (hf * scale * gain.astype(F32)).astype(BF)

    lane = iota((B, 128), 1)
    low = lane < HEAD

    def rope(x, cosv, sinv):
        rot = jnp.where((lane % HEAD) < HEAD // 2, pltpu.roll(x, 128 - HEAD // 2, 1), pltpu.roll(x, HEAD // 2, 1))
        return (x * cosv + rot * sinv).astype(BF).astype(F32)

    pack_send(0)
    for cp in smalls:
        cp.wait()
    lenv = jnp.zeros((B, 128), jnp.int32)
    rowi = iota((B, 128), 0)
    for b in range(B):
        lenv = jnp.where(rowi == b, lens_s[b], lenv)
    freq = jnp.exp((lane % (HEAD // 2)).astype(F32) * (-2.0 * math.log(THETA) / HEAD))
    ang = lenv.astype(F32) * freq
    cosv = jnp.cos(ang)
    sinv = jnp.sin(ang)
    sinv = jnp.where((lane % HEAD) < HEAD // 2, -sinv, sinv)

    row64 = iota((64, 128), 0)
    rowb = row64 % B
    col = iota((64, 128), 1)
    pos = (col // 32) * LOCAL + col % LOCAL
    same = ((col // LOCAL) % 2) == (row64 // 32)
    len64 = jnp.concatenate([lenv] * 4, axis=0)
    valid = same & (pos <= len64)
    isnew = same & (pos == len64)

    def attention(l, h):
        a = rms(h, ga_b[l:l + 1, :])
        for cp in proj_in(l):
            cp.wait()
        q = dot(a, wq_b[l])
        k = rope(dot(a, wk_b[l]), cosv, sinv)
        v = dot(a, wv_b[l]).astype(BF).astype(F32)
        new0 = jnp.where(low, k, pltpu.roll(v, HEAD, 1))
        new1 = jnp.where(low, pltpu.roll(k, HEAD, 1), v)
        kvn[l, 0] = new0
        kvn[l, 1] = new1
        qs = []
        for i in range(2):
            qi = rope(q[:, i * 128:(i + 1) * 128], cosv, sinv)
            qs.append(jnp.where(low, qi, 0.0))
            qs.append(jnp.where(low, pltpu.roll(qi, HEAD, 1), 0.0))
        qf = jnp.concatenate(qs, axis=0)
        newr = jnp.concatenate([new0, new0, new1, new1], axis=0)
        qb = qf.astype(BF)
        snew = jnp.sum(qf * newr, axis=1, keepdims=True)
        s = jnp.zeros((64, 128), F32)
        for c in range(CHUNKS):
            for j in (1, 2, 3):
                kv_recv(l, c, j).wait_recv()
            for b in range(c * CB, (c + 1) * CB, 2):
                kvb = recv[l, b:b + 2].reshape(256, 128)
                sb = dot_nt(qb, kvb)
                s = jnp.where(rowb == b, sb[:, :128], s)
                s = jnp.where(rowb == b + 1, sb[:, 128:], s)
        s = jnp.where(isnew, snew, s) * (HEAD ** -0.5)
        s = jnp.where(valid, s, -1e30)
        e = jnp.exp(s - jnp.max(s, axis=1, keepdims=True))
        p = (e / jnp.sum(e, axis=1, keepdims=True)).astype(BF).astype(F32)
        pn = jnp.sum(jnp.where(isnew, p, 0.0), axis=1, keepdims=True)
        p = jnp.where(isnew, 0.0, p)
        o = pn * newr
        for b in range(0, B, 2):
            pb = jnp.concatenate([jnp.where(rowb == b, p, 0.0), jnp.where(rowb == b + 1, p, 0.0)], axis=1).astype(BF)
            o = o + dot(pb, recv[l, b:b + 2].reshape(256, 128))
        att = jnp.concatenate(
            [jnp.where(low, pltpu.roll(o[32 * i:32 * i + 16], HEAD, 1), o[32 * i + 16:32 * i + 32]) for i in range(2)],
            axis=1).astype(BF)
        for n in range(NCH):
            ar_send(2 * l, n, dot(att, wo_b[l, :, n * NW:(n + 1) * NW]))

    def write_caches(l):
        row = iota((SEQ, 128), 0)

        def body(b, carry):
            kvb = recv[l, b].astype(F32)
            for g in range(2):
                x = kvb[:, g].reshape(SEQ, 128)
                x = jnp.where(row == lens_s[b], kvn[l, g, pl.ds(b, 1), :], x)
                istage[pl.ds(g, SEQ, stride=2), :] = x
            z = istage[...]
            outs[l][0][b] = z[:, :HEAD].astype(BF)
            outs[l][1][b] = z[:, HEAD:].astype(BF)
            return carry

        lax.fori_loop(0, B, body, 0)

    def gates(l, m):
        choice = cho_b[l]
        onehot = jnp.zeros((EXPERTS, B), F32)
        erow = iota((EXPERTS, B), 0)
        for j in range(8):
            onehot = onehot + (erow == choice[j:j + 1, :]).astype(F32)
        eye = (iota((B, B), 0) == iota((B, B), 1)).astype(BF)
        mask = dot_nt(eye, onehot.astype(BF)) > 0.5
        logits = jnp.where(mask, dot_nt(m, wr_b[l]), -1e30)
        ex = jnp.where(mask, jnp.exp(logits - jnp.max(logits, axis=1, keepdims=True)), 0.0)
        return ex / jnp.sum(ex, axis=1, keepdims=True)

    def experts(l, h1):
        m = rms(h1, gm_b[l:l + 1, :])
        gate = gates(l, m)
        for c in range(WCH):
            for cp in expert_in(l, c):
                cp.wait()
        for e in range(EXPERTS):
            acc = None
            for kk in range(4):
                ks = slice(kk * 256, (kk + 1) * 256)
                w = jnp.concatenate([wg_b[l, e, ks, :], wu_b[l, e, ks, :]], axis=1)
                t = dot(m[:, ks], w)
                acc = t if acc is None else acc + t
            ga_act, up = acc[:, :128], acc[:, 128:]
            act = ga_act * jax.nn.sigmoid(ga_act) * up * gate[:, e:e + 1]
            ub[:, e * 128:(e + 1) * 128] = act.astype(BF)
        for n in range(NCH):
            ar_send(2 * l + 1, n, dot(ub[...], wd_b[l, :, n * NW:(n + 1) * NW]))

    h = hid_b[...]
    for l in range(LAYERS):
        attention(l, h)
        if l == 0:
            pack_send(1)
        write_caches(l)
        h1 = ar_sum(2 * l, h)
        experts(l, h1)
        h = ar_sum(2 * l + 1, h1)
    hst[...] = h
    for l in range(LAYERS):
        for c in range(CHUNKS):
            for j in (1, 2, 3):
                kv_send(l, c, j).wait_send()
        for a in (2 * l, 2 * l + 1):
            for n in range(NCH):
                for j in (1, 2, 3):
                    ar_copy(a, n, j, me).wait_send()


def write_out(*refs):
    srcs, dsts, sem = refs[:5], refs[5:10], refs[10]
    copies = [pltpu.make_async_copy(s, d, sem.at[i]) for i, (s, d) in enumerate(zip(srcs, dsts))]
    for cp in copies:
        cp.start()
    for cp in copies:
        cp.wait()


def solution(mesh):
    seq_spec = P('dp', 'tp', None, None)
    head_spec = P('dp', None, 'tp', None)
    col_spec = P(None, None, 'tp')
    ff_spec = P(None, None, None, 'tp')
    anyspec = pl.BlockSpec(memory_space=pl.ANY)
    dma = pltpu.SemaphoreType.DMA

    def local_step(hidden, lengths, choice, keys_one, vals_one, keys_two, vals_two, g_attn, w_q, w_k, w_v, w_o, g_mlp, w_router, w_gate, w_up, w_down):
        cho = jnp.transpose(choice, (0, 2, 1))
        wr = jnp.transpose(w_router, (0, 2, 1))
        wd = w_down.reshape(LAYERS, EXPERTS * 128, D)
        shapes = ((B, D),) + ((B, SEQ * 2, HEAD),) * 4
        results = pl.pallas_call(
            kernel,
            out_shape=tuple(pltpu.VMEM(s, BF) for s in shapes),
            in_specs=[anyspec] * 17,
            out_specs=(pl.BlockSpec(memory_space=pltpu.VMEM),) * 5,
            scratch_shapes=[
                pltpu.SMEM((B,), jnp.int32),
                pltpu.VMEM((B, D), BF),
                pltpu.VMEM((LAYERS, 8, B), jnp.int32),
                pltpu.VMEM((LAYERS, D), BF),
                pltpu.VMEM((LAYERS, D), BF),
                pltpu.VMEM((LAYERS, D, 256), BF),
                pltpu.VMEM((LAYERS, D, 128), BF),
                pltpu.VMEM((LAYERS, D, 128), BF),
                pltpu.VMEM((LAYERS, 256, D), BF),
                pltpu.VMEM((LAYERS, EXPERTS, D), BF),
                pltpu.VMEM((LAYERS, EXPERTS, D, 128), BF),
                pltpu.VMEM((LAYERS, EXPERTS, D, 128), BF),
                pltpu.VMEM((LAYERS, EXPERTS * 128, D), BF),
                pltpu.VMEM((LAYERS, 2, B, LOCAL, 8, HEAD), BF),
                pltpu.VMEM((CB * LOCAL * 8, 128), F32),
                pltpu.VMEM((LAYERS, TP, B, 2, LOCAL, 128), BF),
                pltpu.VMEM((LAYERS, B, TP, 2, LOCAL, 128), BF),
                pltpu.VMEM((2 * SEQ, 128), F32),
                pltpu.VMEM((LAYERS, 2, B, 128), F32),
                pltpu.VMEM((2 * LAYERS, TP, NCH, B, NW), BF),
                pltpu.VMEM((B, EXPERTS * 128), BF),
                dma((6,)),
                dma((LAYERS, 2, CHUNKS)),
                dma((LAYERS, 4)),
                dma((LAYERS, 3, WCH)),
                dma((LAYERS, CHUNKS, 3)),
                dma((LAYERS, CHUNKS, 3)),
                dma((2 * LAYERS, NCH, 3)),
                dma((2 * LAYERS, NCH, 3)),
            ],
            compiler_params=pltpu.CompilerParams(collective_id=0, has_side_effects=True, vmem_limit_bytes=63_500_000),
            name='decode_two_layers',
        )(lengths, hidden, cho, keys_one, vals_one, keys_two, vals_two, g_attn, w_q, w_k, w_v, w_o, g_mlp, wr, w_gate, w_up, wd)
        h, k1, v1, k2, v2 = pl.pallas_call(
            write_out,
            out_shape=tuple(jax.ShapeDtypeStruct(s, BF) for s in shapes),
            in_specs=[pl.BlockSpec(memory_space=pltpu.VMEM)] * 5,
            out_specs=(anyspec,) * 5,
            scratch_shapes=[dma((5,))],
            compiler_params=pltpu.CompilerParams(vmem_limit_bytes=1_000_000),
            name='write_out',
        )(*results)
        shape = (B, SEQ, 2, HEAD)
        return (h, k1.reshape(shape), v1.reshape(shape), k2.reshape(shape), v2.reshape(shape))

    return jax.shard_map(local_step, mesh=mesh, in_specs=(P('dp', None), P('dp'), P(None, 'dp', None), seq_spec, seq_spec, seq_spec, seq_spec, P(), col_spec, col_spec, col_spec, P(None, 'tp', None), P(), P(), ff_spec, ff_spec, P(None, None, 'tp', None)), out_specs=(P('dp', None), head_spec, head_spec, head_spec, head_spec), check_vma=False)
```

```python
import math

import jax
import jax.numpy as jnp
from jax import lax
from jax.experimental import pallas as pl
from jax.experimental.pallas import tpu as pltpu
from jax.sharding import PartitionSpec as P

EPS = 1e-5
THETA = 1000000.0
LAYERS = 2
B = 16
SEQ = 64
D = 1024
HEAD = 64
EXPERTS = 32
TP = 4
LOCAL = SEQ // TP
CHUNKS = 4
CB = B // CHUNKS
WCH = 8
EPC = EXPERTS // WCH
NCH = 4
NW = D // NCH
BF = jnp.bfloat16
F32 = jnp.float32
MESH = pl.DeviceIdType.MESH
NT = (((1,), (1,)), ((), ()))


def dot(a, b):
    return jnp.dot(a, b, preferred_element_type=F32)


def dot_nt(a, b):
    return lax.dot_general(a, b, NT, preferred_element_type=F32)


def iota(shape, dim):
    return lax.broadcasted_iota(jnp.int32, shape, dim)


def kernel(lens, hid, cho, k1, v1, k2, v2, ga, wq, wk, wv, wo, gm, wr, wg, wu, wd,
           hst, ko1, vo1, ko2, vo2,
           lens_s, hid_b, cho_b, g_b, proj_b, wr_b, exp_b,
           kin, stage, send, recv, istage, kvn, ar, ub,
           sm, cs, ws, es, ss, rs, ass, ars):
    me = lax.axis_index('tp')
    peers = {1: me + 1 - 2 * (me % 2), 2: (me + 2) % 4, 3: 3 - me}
    caches = ((k1, v1), (k2, v2))
    outs = ((ko1, vo1), (ko2, vo2))

    def cache_in(l, kv, c):
        return pltpu.make_async_copy(caches[l][kv].at[pl.ds(c * CB, CB)], kin.at[l, c, kv], cs.at[c if l == 0 else CHUNKS])

    def all_of(ref, sem):
        return pltpu.make_async_copy(ref, ref, sem)

    smalls = [pltpu.make_async_copy(s, d, sm.at[min(i, 4)]) for i, (s, d) in enumerate(
        ((lens, lens_s), (hid, hid_b), (cho, cho_b), (wr, wr_b), (ga, g_b.at[0]), (gm, g_b.at[1])))]

    def proj_in(l):
        cols = [pl.ds(i * 128, 128) for i in range(8)]
        pairs = [(wk.at[l], proj_b.at[l, 2]), (wv.at[l], proj_b.at[l, 3])]
        pairs += [(wq.at[l, :, cols[i]], proj_b.at[l, i]) for i in range(2)]
        pairs += [(wo.at[l, :, cols[i]], proj_b.at[l, 4 + i // 4, pl.ds(i % 4 * 256, 256)]) for i in range(8)]
        return [pltpu.make_async_copy(s, d, ws.at[l]) for s, d in pairs]

    def proj_wait(l):
        all_of(proj_b.at[l], ws.at[l]).wait()

    def wo_col(l, i):
        return proj_b[l, 4 + i // 4, i % 4 * 256:(i % 4 + 1) * 256, :]

    def expert_in(l, c):
        rows = EPC * D
        sl = pl.ds(c * rows, rows)
        down = exp_b.at[l, 2, pl.ds(c * EXPERTS * 128, EXPERTS * 128)]
        return [pltpu.make_async_copy(wg.at[l, sl], exp_b.at[l, 0, sl], es.at[l]),
                pltpu.make_async_copy(wu.at[l, sl], exp_b.at[l, 1, sl], es.at[l]),
                pltpu.make_async_copy(wd.at[l, :, pl.ds(c * 128, 128)], down, es.at[l])]

    def expert_wait(l):
        all_of(exp_b.at[l], es.at[l]).wait()

    for c in range(CHUNKS):
        for kv in range(2):
            cache_in(0, kv, c).start()
    for cp in smalls + proj_in(0):
        cp.start()
    bar = pltpu.get_barrier_semaphore()
    for j in (1, 2, 3):
        pl.semaphore_signal(bar, inc=1, device_id={'tp': peers[j]}, device_id_type=MESH)
    for c in range(CHUNKS):
        for kv in range(2):
            cache_in(1, kv, c).start()
    with jax.named_scope('barrier'):
        pl.semaphore_wait(bar, 3)

    def kv_send(l, c, j):
        sl = pl.ds(c * CB, CB)
        return pltpu.make_async_remote_copy(
            send.at[l, peers[j], sl], recv.at[l, sl, me], ss, rs.at[c if l == 0 else CHUNKS],
            device_id={'tp': peers[j]}, device_id_type=MESH)

    def kv_wait(l, c, n):
        all_of(recv.at[l, pl.ds(c * CB, n * CB), pl.ds(0, 3)], rs.at[c if l == 0 else CHUNKS]).wait()

    def start_sends(l, c):
        for j in (2, 3, 1):
            kv_send(l, c, j).start()

    def pack(l):
        for c in range(CHUNKS):
            if l == 0:
                all_of(kin.at[l, c], cs.at[c]).wait()
            elif c == 0:
                all_of(kin.at[l], cs.at[CHUNKS]).wait()
            sl = pl.ds(c * CB, CB)
            kf = kin[l, c, 0].astype(F32).reshape(CB * LOCAL * 8, HEAD)
            vf = kin[l, c, 1].astype(F32).reshape(CB * LOCAL * 8, HEAD)
            stage[...] = jnp.concatenate([kf, vf], axis=1)
            for h in range(8):
                rows = stage[pl.ds(h, CB * LOCAL, stride=8), :].astype(BF)
                send[l, h // 2, sl, h % 2] = rows.reshape(CB, LOCAL, 128)
            recv[l, sl, me] = send[l, me, sl]
            if l == 0:
                start_sends(l, c)

    def ars_of(a, n):
        return ars.at[a // 2, n + 1 if a % 2 else 0]

    def ar_start(a, n, width):
        for j in (2, 3, 1):
            sl = pl.ds(n, width)
            pltpu.make_async_remote_copy(
                ar.at[a, me, sl], ar.at[a, me, sl], ass, ars_of(a, n),
                device_id={'tp': peers[j]}, device_id_type=MESH).start()

    def ar_sum(a, h, width):
        parts = []
        for n in range(NCH):
            if n % width == 0:
                all_of(ar.at[a, pl.ds(0, 3), pl.ds(n, width)], ars_of(a, n)).wait()
            tot = ar[a, 0, n].astype(F32)
            for s in range(1, TP):
                tot = tot + ar[a, s, n].astype(F32)
            parts.append(tot)
        return (h.astype(F32) + jnp.concatenate(parts, axis=1)).astype(BF)

    def rms(h, gain):
        hf = h.astype(F32)
        scale = lax.rsqrt(jnp.mean(hf * hf, axis=1, keepdims=True) + EPS)
        return (hf * scale * gain.astype(F32)).astype(BF)

    lane = iota((B, 128), 1)
    low = lane < HEAD

    def rope(x, cosv, sinv):
        rot = jnp.where((lane % HEAD) < HEAD // 2, pltpu.roll(x, 128 - HEAD // 2, 1), pltpu.roll(x, HEAD // 2, 1))
        return (x * cosv + rot * sinv).astype(BF).astype(F32)

    with jax.named_scope('pack0'):
        pack(0)
    for l in range(LAYERS):
        for c in range(WCH):
            for cp in expert_in(l, c):
                cp.start()
        if l == 0:
            for cp in proj_in(1):
                cp.start()
    with jax.named_scope('pack1'):
        pack(1)
    for cp in smalls[:4]:
        cp.wait()
    all_of(g_b, sm.at[4]).wait()
    lenv = jnp.zeros((B, 128), jnp.int32)
    rowi = iota((B, 128), 0)
    for b in range(B):
        lenv = jnp.where(rowi == b, lens_s[b], lenv)
    freq = jnp.exp((lane % (HEAD // 2)).astype(F32) * (-2.0 * math.log(THETA) / HEAD))
    ang = lenv.astype(F32) * freq
    cosv = jnp.cos(ang)
    sinv = jnp.sin(ang)
    sinv = jnp.where((lane % HEAD) < HEAD // 2, -sinv, sinv)

    row64 = iota((64, 128), 0)
    rowb = row64 % B
    col = iota((64, 128), 1)
    pos = (col // 32) * LOCAL + col % LOCAL
    same = ((col // LOCAL) % 2) == (row64 // 32)
    len64 = jnp.concatenate([lenv] * 4, axis=0)
    valid = same & (pos <= len64)
    isnew = same & (pos == len64)
    keep = len64 >= 0
    wide_keep = jnp.concatenate([lenv, lenv], axis=1) >= 0

    def attention(l, h):
        a = rms(h, g_b[0, l:l + 1, :])
        q, kv = jnp.zeros((B, 256), F32), jnp.zeros((B, 256), F32)
        for kk in range(4):
            ks = slice(kk * 256, (kk + 1) * 256)
            kv = kv + dot(a[:, ks], jnp.concatenate([proj_b[l, 2, ks, :], proj_b[l, 3, ks, :]], axis=1))
            q = q + dot(a[:, ks], jnp.concatenate([proj_b[l, 0, ks, :], proj_b[l, 1, ks, :]], axis=1))
        k = rope(kv[:, :128], cosv, sinv)
        v = kv[:, 128:].astype(BF).astype(F32)
        new0 = jnp.where(low, k, pltpu.roll(v, HEAD, 1))
        new1 = jnp.where(low, pltpu.roll(k, HEAD, 1), v)
        kvn[l, 0] = new0
        kvn[l, 1] = new1
        qs = []
        for i in range(2):
            qi = rope(q[:, i * 128:(i + 1) * 128], cosv, sinv)
            qs.append(jnp.where(low, qi, 0.0))
            qs.append(jnp.where(low, pltpu.roll(qi, HEAD, 1), 0.0))
        qf = jnp.concatenate(qs, axis=0)
        newr = jnp.concatenate([new0, new0, new1, new1], axis=0)
        qb = qf.astype(BF)
        snew = jnp.sum(qf * newr, axis=1, keepdims=True)
        s = jnp.zeros((64, 128), F32)
        for c in range(CHUNKS):
            if l == 0:
                kv_wait(l, c, 1)
                if c == 1:
                    start_sends(1, 0)
            for b in range(c * CB, (c + 1) * CB, 2):
                kvb = recv[l, b:b + 2].reshape(256, 128)
                sb = dot_nt(qb, kvb)
                s = jnp.where(rowb == b, sb[:, :128], s)
                s = jnp.where(rowb == b + 1, sb[:, 128:], s)
        s = jnp.where(isnew, snew, s) * (HEAD ** -0.5)
        s = jnp.where(valid, s, -1e30)
        e = jnp.exp(s - jnp.max(s, axis=1, keepdims=True))
        p = (e / jnp.sum(e, axis=1, keepdims=True)).astype(BF).astype(F32)
        pn = jnp.sum(jnp.where(isnew, p, 0.0), axis=1, keepdims=True)
        p = jnp.where(isnew, 0.0, p)
        halves = [pn * newr, jnp.zeros((64, 128), F32)]
        for b in range(0, B, 2):
            pb = jnp.concatenate([jnp.where(rowb == b, p, 0.0), jnp.where(rowb == b + 1, p, 0.0)], axis=1).astype(BF)
            i = b // 2 % 2
            halves[i] = halves[i] + dot(pb, recv[l, b:b + 2].reshape(256, 128))
        o = halves[0] + jnp.where(keep, halves[1], 0.0)
        att = jnp.concatenate(
            [jnp.where(low, pltpu.roll(o[32 * i:32 * i + 16], HEAD, 1), o[32 * i + 16:32 * i + 32]) for i in range(2)],
            axis=1).astype(BF)
        with jax.named_scope('oproj'):
            outs_n = [dot(att, jnp.concatenate([wo_col(l, 2 * n), wo_col(l, 2 * n + 1)], axis=1)) for n in range(NCH)]
            for n in range(NCH):
                ar[2 * l, me, n] = outs_n[n].astype(BF)
            ar_start(2 * l, 0, NCH)

    def write_caches(l, lo, hi):
        row = iota((SEQ, 128), 0)

        def write_row(b, carry):
            kvb = recv[l, b].astype(F32)
            for g in range(2):
                x = kvb[:, g].reshape(SEQ, 128)
                x = jnp.where(row == lens_s[b], kvn[l, g, pl.ds(b, 1), :], x)
                istage[pl.ds(g, SEQ, stride=2), :] = x
            z = istage[...]
            outs[l][0][b] = z[:, :HEAD].astype(BF)
            outs[l][1][b] = z[:, HEAD:].astype(BF)
            return carry

        lax.fori_loop(lo, hi, write_row, 0)

    def chosen(l):
        choice = cho_b[l]
        onehot = jnp.zeros((EXPERTS, B), F32)
        erow = iota((EXPERTS, B), 0)
        for j in range(8):
            onehot = onehot + (erow == choice[j:j + 1, :]).astype(F32)
        eye = (iota((B, B), 0) == iota((B, B), 1)).astype(BF)
        return dot_nt(eye, onehot.astype(BF))

    def gates(l, m, mask):
        mask = mask > 0.5
        logits = jnp.where(mask, dot_nt(m, wr_b[l]), -1e30)
        ex = jnp.where(mask, jnp.exp(logits - jnp.max(logits, axis=1, keepdims=True)), 0.0)
        return ex / jnp.sum(ex, axis=1, keepdims=True)

    def experts(l, h1, mask):
        m = rms(h1, g_b[1, l:l + 1, :])
        gate = gates(l, m, mask)
        for e in range(EXPERTS):
            acc = None
            for kk in range(4):
                ks = slice(kk * 256, (kk + 1) * 256)
                rows = slice(e * D + kk * 256, e * D + (kk + 1) * 256)
                t = dot(m[:, ks], jnp.concatenate([exp_b[l, 0, rows, :], exp_b[l, 1, rows, :]], axis=1))
                acc = t if acc is None else acc + t
            ga_act, up = acc[:, :128], acc[:, 128:]
            act = ga_act * jax.nn.sigmoid(ga_act) * up * gate[:, e:e + 1]
            ub[e] = act.astype(BF)
        with jax.named_scope('down'):
            us = [jnp.concatenate([ub[2 * i], ub[2 * i + 1]], axis=1) for i in range(16)]
            for n in range(NCH):
                halves = [None, None]
                for i in range(16):
                    rows = [slice(c * EXPERTS * 128 + i * 256, c * EXPERTS * 128 + (i + 1) * 256) for c in (2 * n, 2 * n + 1)]
                    t = dot(us[i], jnp.concatenate([exp_b[l, 2, rl, :] for rl in rows], axis=1))
                    halves[i % 2] = t if halves[i % 2] is None else halves[i % 2] + t
                ar[2 * l + 1, me, n] = (jnp.where(wide_keep, halves[0], 0.0) + halves[1]).astype(BF)
                ar_start(2 * l + 1, n, 1)

    h = hid_b[...]
    for l in range(LAYERS):
        proj_wait(l)
        if l == 1:
            kv_wait(l, 0, CHUNKS)
        with jax.named_scope('attention%d' % l):
            attention(l, h)
        mask = chosen(l)
        with jax.named_scope('write_caches'):
            write_caches(l, 0, B // 2)
            if l == 0:
                for c in range(1, CHUNKS):
                    start_sends(1, c)
            write_caches(l, B // 2, B)
        expert_wait(l)
        with jax.named_scope('sum_att'):
            h1 = ar_sum(2 * l, h, NCH)
        with jax.named_scope('experts%d' % l):
            experts(l, h1, mask)
        with jax.named_scope('sum_moe'):
            h = ar_sum(2 * l + 1, h1, 1)
    hst[...] = h
    all_of(send.at[:, pl.ds(0, 3)], ss).wait()
    all_of(ar.at[:, pl.ds(0, 3)], ass).wait()


def write_out(*refs):
    srcs, dsts, sem = refs[:5], refs[5:10], refs[10]
    for s, d, n, i in zip(srcs, dsts, (1, 4, 4, 4, 4), range(5)):
        rows = B // n
        for c in range(n):
            pltpu.make_async_copy(s.at[pl.ds(c * rows, rows)], d.at[pl.ds(c * rows, rows)], sem.at[i]).start()
    for s, d, i in zip(srcs, dsts, range(5)):
        pltpu.make_async_copy(s, d, sem.at[i]).wait()


def solution(mesh):
    seq_spec = P('dp', 'tp', None, None)
    head_spec = P('dp', None, 'tp', None)
    col_spec = P(None, None, 'tp')
    ff_spec = P(None, None, None, 'tp')
    anyspec = pl.BlockSpec(memory_space=pl.ANY)
    dma = pltpu.SemaphoreType.DMA

    def local_step(hidden, lengths, choice, keys_one, vals_one, keys_two, vals_two, g_attn, w_q, w_k, w_v, w_o, g_mlp, w_router, w_gate, w_up, w_down):
        cho = jnp.transpose(choice, (0, 2, 1))
        wr = jnp.transpose(w_router, (0, 2, 1))
        wd = w_down.reshape(LAYERS, EXPERTS * 128, D)
        wg = w_gate.reshape(LAYERS, EXPERTS * D, 128)
        wu = w_up.reshape(LAYERS, EXPERTS * D, 128)
        shapes = ((B, D),) + ((B, SEQ * 2, HEAD),) * 4
        results = pl.pallas_call(
            kernel,
            out_shape=tuple(pltpu.VMEM(s, BF) for s in shapes),
            in_specs=[anyspec] * 17,
            out_specs=(pl.BlockSpec(memory_space=pltpu.VMEM),) * 5,
            scratch_shapes=[
                pltpu.SMEM((B,), jnp.int32),
                pltpu.VMEM((B, D), BF),
                pltpu.VMEM((LAYERS, 8, B), jnp.int32),
                pltpu.VMEM((2, LAYERS, D), BF),
                pltpu.VMEM((LAYERS, 6, D, 128), BF),
                pltpu.VMEM((LAYERS, EXPERTS, D), BF),
                pltpu.VMEM((LAYERS, 3, EXPERTS * D, 128), BF),
                pltpu.VMEM((LAYERS, CHUNKS, 2, CB, LOCAL, 8, HEAD), BF),
                pltpu.VMEM((CB * LOCAL * 8, 128), F32),
                pltpu.VMEM((LAYERS, TP, B, 2, LOCAL, 128), BF),
                pltpu.VMEM((LAYERS, B, TP, 2, LOCAL, 128), BF),
                pltpu.VMEM((2 * SEQ, 128), F32),
                pltpu.VMEM((LAYERS, 2, B, 128), F32),
                pltpu.VMEM((2 * LAYERS, TP, NCH, B, NW), BF),
                pltpu.VMEM((EXPERTS, B, 128), BF),
                dma((5,)),
                dma((CHUNKS + 1,)),
                dma((LAYERS,)),
                dma((LAYERS,)),
                dma,
                dma((CHUNKS + 1,)),
                dma,
                dma((LAYERS, NCH + 1)),
            ],
            compiler_params=pltpu.CompilerParams(collective_id=0, has_side_effects=True, vmem_limit_bytes=63_500_000),
            name='decode_two_layers',
        )(lengths, hidden, cho, keys_one, vals_one, keys_two, vals_two, g_attn, w_q, w_k, w_v, w_o, g_mlp, wr, wg, wu, wd)
        h, k1, v1, k2, v2 = pl.pallas_call(
            write_out,
            out_shape=tuple(jax.ShapeDtypeStruct(s, BF) for s in shapes),
            in_specs=[pl.BlockSpec(memory_space=pltpu.VMEM)] * 5,
            out_specs=(anyspec,) * 5,
            scratch_shapes=[dma((5,))],
            compiler_params=pltpu.CompilerParams(vmem_limit_bytes=1_000_000),
            name='write_out',
        )(*results)
        shape = (B, SEQ, 2, HEAD)
        return (h, k1.reshape(shape), v1.reshape(shape), k2.reshape(shape), v2.reshape(shape))

    return jax.shard_map(local_step, mesh=mesh, in_specs=(P('dp', None), P('dp'), P(None, 'dp', None), seq_spec, seq_spec, seq_spec, seq_spec, P(), col_spec, col_spec, col_spec, P(None, 'tp', None), P(), P(), ff_spec, ff_spec, P(None, None, 'tp', None)), out_specs=(P('dp', None), head_spec, head_spec, head_spec, head_spec), check_vma=False)
```
